64 devices in a mesh: dp: 4 (over x, y), tp: 16 (over z, core).
Axes of the slice: x: 2, y: 2, z: 8, core: 2. Of those that a mesh axis runs over, the one named last changes fastest.
The devices are a block of a 4x4x8 slice.
Arguments:
- x_in: bfloat16 [16384, 4096], P(('dp', 'tp')), parts along dimension 0
- w_in: bfloat16 [4096, 11008], P(None, 'tp')
- grad_out: bfloat16 [16384, 11008], P('dp', 'tp'), parts along dimension 0
Outputs:
- output 1: bfloat16 [16384, 4096], P(('dp', 'tp')), parts along dimension 0
- output 2: float32 [16384, 11008], P('dp', 'tp'), parts along dimension 0
There are 4 independent parts. The reference program is written for one: setup_inputs(seed, part) draws one part's arguments, and reference() takes and returns one part's arrays. A program takes and returns all parts, laid end to end along the dimension named above; an argument that names none is the same for every part.
All inputs are finite; a program needn't handle non-finite values.
Results may differ from the reference program's by a relative error of at most 0.001.
Values are sent between devices in bfloat16 or wider.
A program may use at most 768 MiB of HBM per device.

```python
import jax
import jax.numpy as jnp

TOKENS = 4096
HIDDEN = 4096
FFN_DIM = 11008


def setup_inputs(seed: int = 0, part: int = 0) -> dict:
    base_key = jax.random.key(seed)
    part_key = jax.random.fold_in(base_key, part)
    key_x, key_grad = jax.random.split(part_key)
    key_weight = jax.random.key(seed + 1)
    x_in = jax.random.normal(key_x, (TOKENS, HIDDEN), jnp.float32).astype(jnp.bfloat16)
    w_in = (jax.random.normal(key_weight, (HIDDEN, FFN_DIM), jnp.float32) * HIDDEN ** -0.5).astype(jnp.bfloat16)
    grad_scale = (HIDDEN / FFN_DIM) ** 0.5
    grad_out = (jax.random.normal(key_grad, (TOKENS, FFN_DIM), jnp.float32) * grad_scale).astype(jnp.bfloat16)
    return {"x_in": x_in, "w_in": w_in, "grad_out": grad_out}


def reference(x_in, w_in, grad_out):
    grad_x = jnp.dot(grad_out, w_in.T, preferred_element_type=jnp.float32).astype(jnp.bfloat16)
    grad_w = jnp.dot(x_in.T, grad_out, preferred_element_type=jnp.float32)
    return (grad_x, grad_w)
```

```python
import jax
import jax.numpy as jnp
from jax import lax
from jax.sharding import PartitionSpec as P


NT = (((1,), (1,)), ((), ()))
TN = (((0,), (0,)), ((), ()))


def solution(mesh):
    n = mesh.shape["tp"]
    ring = n // 2
    sibling = [(i, i ^ 1) for i in range(n)]
    up = [(i, (i + 2) % n) for i in range(n)]
    down = [(i, (i - 2) % n) for i in range(n)]

    def per_device(x_blk, w_blk, grad_blk):
        tokens, hidden = x_blk.shape
        half = hidden // 2
        me = lax.axis_index("tp")
        core, chip = me & 1, me >> 1

        def rows_of(which):
            return jnp.concatenate(
                [lax.dynamic_slice_in_dim(grad_blk, (2 * k + which) * tokens, tokens, 0) for k in range(ring)], axis=0
            )

        xs = [x_blk[:, :half], x_blk[:, half:]]
        perms = ((up, -1), (down, 1))
        xs = [lax.ppermute(xs[p], "tp", perms[p][0]) for p in range(2)]

        g_cat = jnp.concatenate([rows_of(core), lax.ppermute(rows_of(1 - core), "tp", sibling)], axis=1)
        w_cat = jnp.concatenate([w_blk, lax.ppermute(w_blk, "tp", sibling)], axis=1)
        x_sib = lax.ppermute(x_blk, "tp", sibling)

        def partial(dest, p):
            g = lax.dynamic_slice_in_dim(g_cat, dest * tokens, tokens, 0)
            return lax.dot_general(g, w_cat[p * half : (p + 1) * half], NT, preferred_element_type=jnp.float32)

        def put(x_full, piece, dest_chip, dest_core, col):
            return lax.dynamic_update_slice(x_full, piece, ((2 * dest_chip + dest_core) * tokens, col))

        x_full = jnp.zeros((n * tokens, hidden), x_blk.dtype)
        x_full = put(x_full, x_blk, chip, core, 0)
        x_full = put(x_full, x_sib, chip, 1 - core, 0)

        sums = [None, None]
        for step in range(1, ring):
            totals = []
            for p, (perm, sign) in enumerate(perms):
                term = partial((chip + sign * step) & (ring - 1), p)
                totals.append(term if step == 1 else sums[p] + term)
            got = xs
            sums = [lax.ppermute(totals[p], "tp", perms[p][0]) for p in range(2)]
            if step < ring - 1:
                xs = [
                    lax.ppermute(lax.optimization_barrier((xs[p], totals[p]))[0], "tp", perms[p][0]) for p in range(2)
                ]
            for p, (_, sign) in enumerate(perms):
                origin = (chip + sign * step) & (ring - 1)
                shared = lax.ppermute(got[p], "tp", sibling)
                x_full = put(x_full, got[p], origin, core, p * half)
                x_full = put(x_full, shared, origin, 1 - core, p * half)
        grad_x = jnp.concatenate([sums[p] + partial(chip, p) for p in range(2)], axis=1)
        grad_w = lax.dot_general(x_full, grad_blk, TN, preferred_element_type=jnp.float32)
        return grad_x.astype(x_blk.dtype), grad_w

    return jax.shard_map(
        per_device,
        mesh=mesh,
        in_specs=(P(("dp", "tp"), None), P(None, "tp"), P("dp", "tp")),
        out_specs=(P(("dp", "tp"), None), P("dp", "tp")),
        check_vma=False,
    )
```

```python
import jax
import jax.numpy as jnp
from jax import lax
from jax.sharding import PartitionSpec as P


NT = (((1,), (1,)), ((), ()))
TN = (((0,), (0,)), ((), ()))
F32 = jnp.float32


def after(value, *others):
    return lax.optimization_barrier((value, *others))[0]


def solution(mesh):
    n = mesh.shape["tp"]
    ring = n // 2
    far = ring // 2
    sibling = [(i, i ^ 1) for i in range(n)]
    perms = ([(i, (i + 2) % n) for i in range(n)], [(i, (i - 2) % n) for i in range(n)])
    signs = (1, -1)
    both = range(2)

    def body(x_blk, w_blk, grad_blk):
        tokens, hidden = x_blk.shape
        half = hidden // 2
        me = lax.axis_index("tp")
        core, chip = me & 1, me >> 1

        def hop(values):
            return [lax.ppermute(values[p], "tp", perms[p]) for p in both]

        def swap(value):
            return lax.ppermute(value, "tp", sibling)

        def chip_at(offset):
            return (chip + offset) & (ring - 1)

        def rows_of(which):
            return [
                lax.dynamic_slice(
                    grad_blk,
                    ((2 * chip_at(j) + which) * tokens, 0),
                    (tokens, grad_blk.shape[1]),
                    allow_negative_indices=False,
                )
                for j in range(1, ring + 1)
            ]

        x_in = [hop([x_blk, x_blk])]

        w_sib = swap(w_blk)
        g_send = jnp.concatenate(rows_of(1 - core), axis=0)
        g_keep = jnp.concatenate(rows_of(core), axis=0)
        g_sib = swap(g_send)
        w_cat = jnp.concatenate([w_blk, w_sib], axis=1)
        g_cat = jnp.concatenate([g_keep, g_sib], axis=1)
        x_sib = swap(x_blk)

        g_far = g_cat[(far - 1) * tokens : far * tokens]
        first = [
            lax.dot_general(g_far, w_cat[p * half : (p + 1) * half], NT, preferred_element_type=F32) for p in both
        ]
        lead = hop(first)
        terms = lax.dot_general(after(g_cat, *first), w_cat, NT, preferred_element_type=F32)

        def term(offset, p):
            j = (offset - 1) % ring
            return terms[j * tokens : (j + 1) * tokens, p * half : (p + 1) * half]

        def put(x_full, piece, origin, which, col):
            return lax.dynamic_update_slice(
                x_full, piece, ((2 * origin + which) * tokens, col), allow_negative_indices=False
            )

        trail_total = [term(signs[p] * (far - 1), 1 - p) for p in both]
        trail = hop(trail_total)
        x_full = jnp.broadcast_to(after(jnp.zeros((), x_blk.dtype), *trail_total), (n * tokens, hidden))
        x_full = put(x_full, x_blk, chip, core, 0)
        x_full = put(x_full, x_sib, chip, 1 - core, 0)
        gate = trail_total
        for step in range(1, far):
            got = [after(x_in[-1][p], *gate) for p in both]
            if step < far - 1:
                x_in.append(hop(got))
            else:
                x_in.append(hop([got[p][:, p * half : (p + 1) * half] for p in both]))
            shared = [swap(got[p]) for p in both]
            for p in both:
                x_full = put(x_full, got[p], chip_at(-signs[p] * step), core, 0)
                x_full = put(x_full, shared[p], chip_at(-signs[p] * step), 1 - core, 0)
            lead_total = [after(lead[p], *got) + term(signs[p] * (far - step), p) for p in both]
            lead = hop(lead_total)
            if step < far - 1:
                trail_total = [after(trail[p], *lead_total) + term(signs[p] * (far - 1 - step), 1 - p) for p in both]
                trail = hop(trail_total)
                gate = trail_total
            else:
                gate = lead_total
        got = [after(x_in[-1][p], *gate) for p in both]
        shared = [swap(got[p]) for p in both]
        for p in both:
            x_full = put(x_full, got[p], chip_at(far), core, p * half)
            x_full = put(x_full, shared[p], chip_at(far), 1 - core, p * half)
        mine = [after(trail[1 - p], *got) + term(0, p) for p in both]
        grad_w = lax.dot_general(x_full, grad_blk, TN, preferred_element_type=F32)
        grad_x = jnp.concatenate([(mine[p] + lead[p]).astype(x_blk.dtype) for p in both], axis=1)
        return grad_x, grad_w

    return jax.shard_map(
        body,
        mesh=mesh,
        in_specs=(P(("dp", "tp"), None), P(None, "tp"), P("dp", "tp")),
        out_specs=(P(("dp", "tp"), None), P("dp", "tp")),
        check_vma=False,
    )
```
